32 devices in a mesh: ep: 32 (over z, y, x, core).
Axes of the slice: x: 2, y: 2, z: 4, core: 2. Of those that a mesh axis runs over, the one named last changes fastest.
Arguments:
- x: bfloat16 [32768, 768], P('ep')
- gate_w: bfloat16 [768, 64], replicated
- up_w: bfloat16 [64, 768, 3072], P('ep')
- down_w: bfloat16 [64, 3072, 768], P('ep')
- expert_picks: int32 [64, 1024], P('ep')
- loss_w: bfloat16 [32768, 768], P('ep')
Outputs:
- output 1: bfloat16 [32768, 768], P('ep')
- output 2: float32 [], replicated
- output 3: bfloat16 [32768, 768], P('ep')
- output 4: bfloat16 [64, 768, 3072], P('ep')
- output 5: bfloat16 [64, 3072, 768], P('ep')
- output 6: float32 [768, 64], replicated
All inputs are finite; a program needn't handle non-finite values.
Results may differ from the reference program's by a relative error of at most 0.0107156.
Values are sent between devices in bfloat16 or wider.
A program may use at most 1 GiB of HBM per device.

```python
import functools
import math
import jax
import jax.numpy as jnp
from jax import lax

HIDDEN = 768
FFN_DIM = 3072
EXPERTS = 64
TOK_DEV = 1024
GROUP_DEVS = 32

TOKENS = TOK_DEV * GROUP_DEVS
CAPACITY = 2 * TOKENS // EXPERTS
LOCAL_EXPERTS = EXPERTS // GROUP_DEVS
SHARD_PICKS = CAPACITY // GROUP_DEVS
POOL_SIZE = max(SHARD_PICKS, LOCAL_EXPERTS * SHARD_PICKS // 2)


@jax.custom_vjp
def grad_to_bf16(in_value):
    return in_value


def grad_to_bf16_fwd(in_value):
    return in_value, None


def grad_to_bf16_bwd(residual, cotangent):
    return (cotangent.astype(jnp.bfloat16).astype(jnp.float32),)


grad_to_bf16.defvjp(grad_to_bf16_fwd, grad_to_bf16_bwd)


def draw_picks(base_key):
    perm_keys = jax.random.split(jax.random.fold_in(base_key, 1), GROUP_DEVS)
    shard_perms = jax.vmap(functools.partial(jax.random.permutation, x=TOK_DEV))(perm_keys)
    offsets = jax.random.randint(jax.random.fold_in(base_key, 2), (GROUP_DEVS, GROUP_DEVS), 0, TOK_DEV)
    pool_pos = (jnp.arange(LOCAL_EXPERTS)[:, None] * SHARD_PICKS + jnp.arange(SHARD_PICKS)[None, :]) % POOL_SIZE
    perm_pos = (offsets[:, None, :, None] + pool_pos[None, :, None, :]) % TOK_DEV
    src_ids = jnp.arange(GROUP_DEVS)[None, None, :, None]
    token_ids = src_ids * TOK_DEV + shard_perms[src_ids, perm_pos]
    return token_ids.reshape(EXPERTS, CAPACITY).astype(jnp.int32)


def setup_inputs(seed: int = 0) -> dict:
    key_list = jax.random.split(jax.random.key(seed), 6)
    x = jax.random.normal(key_list[0], (TOKENS, HIDDEN), jnp.float32)
    gate_w = jax.random.normal(key_list[1], (HIDDEN, EXPERTS), jnp.float32) * HIDDEN ** -0.5
    up_w = jax.random.normal(key_list[2], (EXPERTS, HIDDEN, FFN_DIM), jnp.float32) * HIDDEN ** -0.5
    down_w = jax.random.normal(key_list[3], (EXPERTS, FFN_DIM, HIDDEN), jnp.float32) * (EXPERTS / (2.0 * math.sqrt(FFN_DIM)))
    loss_w = jax.random.normal(key_list[5], (TOKENS, HIDDEN), jnp.float32)
    return {'x': x.astype(jnp.bfloat16), 'gate_w': gate_w.astype(jnp.bfloat16), 'up_w': up_w.astype(jnp.bfloat16), 'down_w': down_w.astype(jnp.bfloat16), 'expert_picks': draw_picks(key_list[4]), 'loss_w': loss_w.astype(jnp.bfloat16)}


def mixed_tokens(x_f32, gate_w32, up_w, down_w, expert_picks):
    logits = grad_to_bf16(jnp.dot(x_f32, gate_w32))
    gate_probs = jax.nn.softmax(logits, axis=-1)
    gate_vals = gate_probs[expert_picks, jnp.arange(EXPERTS)[:, None]]

    def one_expert(operands):
        pick_ids, up_one, down_one, gate_one = operands
        tok_rows = grad_to_bf16(x_f32[pick_ids])
        pre_act = grad_to_bf16(jnp.dot(tok_rows, up_one.astype(jnp.float32)))
        hidden_act = jax.nn.gelu(pre_act).astype(jnp.bfloat16)
        expert_out = jnp.dot(hidden_act.astype(jnp.float32), down_one.astype(jnp.float32)).astype(jnp.bfloat16)
        return gate_one[:, None] * expert_out.astype(jnp.float32)

    contrib = lax.map(jax.checkpoint(one_expert), (expert_picks, up_w, down_w, gate_vals))
    return x_f32.at[expert_picks.reshape(-1)].add(contrib.reshape(-1, HIDDEN))


def reference(x, gate_w, up_w, down_w, expert_picks, loss_w):
    loss_scale = 1.0 / math.sqrt(TOKENS * HIDDEN)
    mixed_f32, pullback = jax.vjp(functools.partial(mixed_tokens, expert_picks=expert_picks), x.astype(jnp.float32), gate_w.astype(jnp.float32), up_w, down_w)
    y = mixed_f32.astype(jnp.bfloat16)
    weight_f32 = loss_w.astype(jnp.float32)
    loss = jnp.sum(y.astype(jnp.float32) * weight_f32) * loss_scale
    grad_x, grad_gate, grad_up, grad_down = pullback(weight_f32 * loss_scale)
    return y, loss, grad_x.astype(jnp.bfloat16), grad_up, grad_down, grad_gate
```

```python
import math
import jax
import jax.numpy as jnp
from jax import lax
from jax.sharding import PartitionSpec as P

F32 = jnp.float32
BF16 = jnp.bfloat16


def split3(v):
    hi = lax.reduce_precision(v, 8, 7)
    rest = v - hi
    mid = lax.reduce_precision(rest, 8, 7)
    return hi.astype(BF16), mid.astype(BF16), (rest - mid).astype(BF16)


def dot(a, b, ca, cb):
    return lax.dot_general(a, b, (((ca,), (cb,)), ((), ())), preferred_element_type=F32)


def solution(mesh):
    group_size = mesh.shape['ep']

    def device_step(x, gate_w, up_w, down_w, expert_picks, loss_w):
        tok_dev, hidden = x.shape
        local_experts, capacity = expert_picks.shape
        shard_picks = capacity // group_size
        experts = gate_w.shape[1]
        loss_scale = 1.0 / math.sqrt(tok_dev * group_size * hidden)
        my_index = lax.axis_index('ep')

        def exchange(rows):
            return lax.all_to_all(rows.reshape(group_size, shard_picks, -1), 'ep', 0, 0, tiled=True).reshape(capacity, -1)

        def softmax_rows(rows):
            return jax.nn.softmax(dot(rows, gate_w, 1, 0), axis=-1)

        ids = lax.all_to_all(expert_picks[0].reshape(group_size, shard_picks), 'ep', 0, 0, tiled=True)
        slot_tok = ids.reshape(-1) - my_index * tok_dev
        pick = (slot_tok[:, None] == jnp.arange(tok_dev)[None, :]).astype(BF16)
        x_out = dot(pick, x, 1, 0).astype(BF16)
        r_out = dot(pick, loss_w, 1, 0).astype(BF16)
        x_in = exchange(x_out)
        r_in = exchange(r_out)

        probs_in = softmax_rows(x_in)
        dy_in = r_in.astype(F32) * loss_scale
        cols = jnp.arange(experts)[None, :]
        kept = []
        for l in range(local_experts):
            gate = jnp.sum(jnp.where(cols == my_index * local_experts + l, probs_in, 0.0), axis=1)
            pre = dot(x_in, up_w[l], 1, 0)
            act, pull = jax.vjp(jax.nn.gelu, pre)
            act = act.astype(BF16)
            h = dot(act, down_w[l], 1, 0).astype(BF16)
            kept.append((gate, act, pull, exchange(h)))

        g_back, grad_up, grad_down = [], [], []
        for l in range(local_experts):
            gate, act, pull, _ = kept[l]
            dh = (gate[:, None] * dy_in).astype(BF16)
            du = dot(dh, down_w[l], 1, 1).astype(BF16)
            da = pull(du.astype(F32))[0].astype(BF16)
            g = dot(da, up_w[l], 1, 1).astype(BF16)
            g_back.append(exchange(g))
            grad_down.append(dot(act, dh, 0, 0).astype(BF16))
            grad_up.append(dot(x_in, da, 0, 0).astype(BF16))

        probs = softmax_rows(x)
        slot_dev = jnp.arange(capacity) // shard_picks
        parts = jnp.concatenate(split3(probs), axis=1)
        slot_probs = dot(pick, parts, 1, 0).reshape(capacity, 3, experts)
        slot_probs = slot_probs[:, 0] + slot_probs[:, 1] + slot_probs[:, 2]
        mixed = 0.0
        d_slot = 0.0
        for l in range(local_experts):
            h_l = kept[l][3].astype(F32)
            here = cols == (slot_dev * local_experts + l)[:, None]
            gate_l = jnp.sum(jnp.where(here, slot_probs, 0.0), axis=1)
            mixed += gate_l[:, None] * h_l
            d_gate = jnp.sum(r_out.astype(F32) * loss_scale * h_l, axis=1)
            d_slot += jnp.where(here, d_gate[:, None], 0.0)
        m1, m2, m3 = split3(mixed)
        y = (x.astype(F32) + (dot(pick, m1, 0, 0) + dot(pick, m2, 0, 0) + dot(pick, m3, 0, 0))).astype(BF16)
        weight = loss_w.astype(F32)
        loss_part = jnp.sum(y.astype(F32) * weight) * loss_scale

        d_parts = dot(pick, jnp.concatenate(split3(d_slot), axis=1), 0, 0).reshape(tok_dev, 3, experts)
        d_probs = d_parts[:, 0] + d_parts[:, 1] + d_parts[:, 2]
        d_logits = (probs * (d_probs - jnp.sum(probs * d_probs, axis=-1, keepdims=True))).astype(BF16)
        gate_part = dot(x, d_logits, 0, 0).reshape(group_size, -1, experts)
        small = jnp.concatenate([gate_part, jnp.broadcast_to(loss_part, (group_size, 1, experts))], axis=1)
        small = jnp.sum(lax.all_to_all(small, 'ep', 0, 0, tiled=True).reshape(group_size, -1, experts), axis=0)
        loss = small[-1, 0]
        grad_gate = lax.all_gather(small[:-1], 'ep', axis=0, tiled=True)

        grad_x = (weight * loss_scale + sum(dot(pick, g, 0, 0) for g in g_back) + dot(d_logits, gate_w, 1, 1)).astype(BF16)
        return y, loss, grad_x, jnp.stack(grad_up), jnp.stack(grad_down), grad_gate

    return jax.shard_map(device_step, mesh=mesh,
                         in_specs=(P('ep'), P(), P('ep'), P('ep'), P('ep'), P('ep')),
                         out_specs=(P('ep'), P(), P('ep'), P('ep'), P('ep'), P()),
                         check_vma=False)
```

```python
import functools
import math
import jax
import jax.numpy as jnp
from jax import lax
from jax.experimental import pallas as pl
from jax.experimental.pallas import tpu as pltpu
from jax.sharding import PartitionSpec as P

F32 = jnp.float32
BF16 = jnp.bfloat16
GROUP = 8
TILE = 512
LANES = 128
C0 = math.sqrt(2.0 / math.pi)
C1 = 0.044715


def dot(a, b, ca=1, cb=0):
    return lax.dot_general(a, b, (((ca,), (cb,)), ((), ())), preferred_element_type=F32)


def split3(v):
    hi = v.astype(BF16)
    rest = v - hi.astype(F32)
    mid = rest.astype(BF16)
    return hi, mid, (rest - mid.astype(F32)).astype(BF16)


def softmax(logits):
    e = jnp.exp(logits - jnp.max(logits, axis=1, keepdims=True))
    return e / jnp.sum(e, axis=1, keepdims=True)


def xor(a, b, bits):
    return sum(((a // (1 << i) + b // (1 << i)) % 2) * (1 << i) for i in range(bits))


def moe_kernel(n, loss_scale, ids, x, r, wg, w1, w2,
               y_out, gx_out, gu_out, gd_out, gg_out, loss_out,
               xr_v, w1_v, w2_v, pick, xr_s, xr_in, hs, h_in, gs, g_in, dh_v, s_in, s_own, u_t, da_t, acc, big, out_st,
               ids_in, ids_t, d_acc, dlog, red_s, red_in, swap_s, swap_in, all_s, all_in,
               load_sem, ids_ss, ids_rs, xr_ss, xr_rs, h_ss, h_rs, g_ss, g_rs, red_ss, red_rs, swap_ss, swap_rs, all_ss, all_rs, out_sem):
    me = lax.axis_index('ep')
    bits = n.bit_length() - 1
    stages = n // GROUP
    half = n // 2
    tok, hidden = xr_v.shape[1:]
    per = tok // n
    rows = GROUP * per
    local_experts, _, ffn = w1_v.shape
    tiles = ffn // TILE
    experts = wg.shape[0]
    most = pl.ds(0, n - 1)

    def peer(p):
        return xor(me, n - 1 - p, bits)

    def group(i):
        return xor(me // GROUP, stages - 1 - i, bits - 3)

    def remote(src, dst, ss, rs, d):
        return pltpu.make_async_remote_copy(src, dst, ss, rs, device_id=(d,), device_id_type=pl.DeviceIdType.MESH)

    def span(q):
        return pl.ds(pl.multiple_of(q * rows, rows), rows)

    loads = [pltpu.make_async_copy(x, xr_v.at[0], load_sem.at[0]), pltpu.make_async_copy(r, xr_v.at[1], load_sem.at[1]),
             pltpu.make_async_copy(w1, w1_v, load_sem.at[2]), pltpu.make_async_copy(w2, w2_v, load_sem.at[3])]
    for c in loads:
        c.start()

    barrier = pltpu.get_barrier_semaphore()

    @pl.loop(0, n - 1)
    def _(p):
        pl.semaphore_signal(barrier, inc=1, device_id=(peer(p),), device_id_type=pl.DeviceIdType.MESH)
    pl.semaphore_wait(barrier, n - 1)

    packed = LANES // per

    @pl.loop(0, n - 1)
    def _(p):
        d = peer(p)
        remote(ids.at[d // packed], ids_in.at[me], ids_ss, ids_rs, d).start()
    ids_in[me] = ids[me // packed]
    all_ids = remote(ids_in.at[most], ids_in.at[most], ids_ss, ids_rs, me)
    all_ids.wait_send()
    all_ids.wait_recv()
    flat = ids_in[...].reshape(n, LANES).astype(F32)
    ids_t[...] = jnp.transpose(jnp.concatenate([flat] * (LANES // n), axis=0))
    cols = ids_t[pl.ds(pl.multiple_of((me % packed) * per, per), per), :]
    lane = lax.broadcasted_iota(jnp.int32, (per, LANES), 1)
    tok_iota = (lax.broadcasted_iota(jnp.int32, (per, tok), 1) + me * tok).astype(F32)

    loads[0].wait()
    loads[1].wait()

    @pl.loop(0, 2 * stages + 1)
    def _(s):
        @pl.when(s < stages)
        def _():
            base = group(s % stages) * GROUP
            for j in range(GROUP):
                col = jnp.sum(jnp.where(lane == base + j, cols, 0.0), axis=1, keepdims=True)
                at = pl.multiple_of((base + j) * per, per)
                pick[pl.ds(at, per), :] = jnp.where(tok_iota == col, 1.0, 0.0).astype(BF16)

        @pl.when(s < 2 * stages)
        def _():
            w, q = s // stages, group(s % stages)
            xr_s[w, pl.ds(q * GROUP, GROUP)] = dot(pick[span(q), :], xr_v[w]).astype(BF16).reshape(GROUP, per, hidden)

        @pl.when(s > 0)
        def _():
            w, i = (s - 1) // stages, (s - 1) % stages

            @pl.loop(0, GROUP)
            def _(j):
                p = i * GROUP + j

                @pl.when(p < n - 1)
                def _():
                    d = peer(p)
                    remote(xr_s.at[w, d], xr_in.at[w, me], xr_ss, xr_rs.at[w * stages + i], d).start()

                @pl.when(p == n - 1)
                def _():
                    xr_in[w, me] = xr_s[w, me]

    @pl.loop(0, stages)
    def _(c):
        s_own[span(c), :] = softmax(dot(xr_v[0, span(c), :], wg[...], 1, 1))
    loads[2].wait()
    loads[3].wait()

    def await_group(ref, sem, i):
        for cond, size in ((i < stages - 1, GROUP), (i == stages - 1, GROUP - 1)):
            @pl.when(cond)
            def _():
                part = ref(pl.ds(group(i) * GROUP, size))
                remote(part, part, xr_ss, sem, me).wait_recv()

    def send_h(i):
        @pl.loop(0, GROUP)
        def _(j):
            p = i * GROUP + j

            @pl.when(p < n - 1)
            def _():
                d = peer(p)
                remote(hs.at[d], h_in.at[me], h_ss, h_rs, d).start()

            @pl.when(p == n - 1)
            def _():
                h_in[me] = hs[me]

    lane_e = lax.broadcasted_iota(jnp.int32, (rows, experts), 1)
    row_dev = lax.broadcasted_iota(jnp.int32, (rows, experts), 0) // per

    @pl.loop(0, stages)
    def _(i):
        q = group(i)
        await_group(lambda b: xr_in.at[0, b], xr_rs.at[i], i)
        xg = xr_in[0, pl.ds(q * GROUP, GROUP)].reshape(rows, hidden)
        s_in[span(q), :] = softmax(dot(xg, wg[...], 1, 1))

        @pl.when(i > 0)
        def _():
            send_h(i - 1)

        @pl.loop(0, local_experts)
        def _(l):
            acc[...] = jnp.zeros_like(acc)

            @pl.loop(0, tiles)
            def _(t):
                at = pl.ds(pl.multiple_of(t * TILE, TILE), TILE)
                a = dot(xg, w1_v[l, :, at])
                u = (0.5 * a * (1.0 + jnp.tanh(C0 * (a + C1 * (a * a * a))))).astype(BF16)
                acc[...] += dot(u, w2_v[l, at, :])
            hs[pl.ds(q * GROUP, GROUP), pl.ds(pl.multiple_of(l * per, per), per), :] = acc[...].astype(BF16).reshape(GROUP, per, hidden)

    @pl.loop(0, stages)
    def _(i):
        await_group(lambda b: xr_in.at[1, b], xr_rs.at[stages + i], i)

        @pl.when(i == 0)
        def _():
            send_h(stages - 1)

    def wide_of(l):
        return pl.ds(pl.multiple_of(l * per, per), per)

    def send_g(l, i, lo, hi):
        @pl.loop(lo, hi)
        def _(j):
            p = i * GROUP + j

            @pl.when(p < n - 1)
            def _():
                d = peer(p)
                remote(gs.at[l, d], g_in.at[l, me], g_ss, g_rs.at[l * stages + i], d).start()

            @pl.when(p == n - 1)
            def _():
                g_in[l, me] = gs[l, me]

    def grads_out(step):
        l, t = step // tiles, step % tiles
        at = pl.ds(pl.multiple_of(t * TILE, TILE), TILE)
        pltpu.make_async_copy(w1_v.at[l, :, at], gu_out.at[l, :, at], out_sem.at[0]).start()
        pltpu.make_async_copy(w2_v.at[l, at, :], gd_out.at[l, at, :], out_sem.at[1]).start()

    @pl.loop(0, local_experts)
    def _(l):
        @pl.loop(0, stages)
        def _(q):
            gate = jnp.sum(jnp.where(lane_e == me * local_experts + l, s_in[span(q), :], 0.0), axis=1, keepdims=True)
            dy = xr_in[1, pl.ds(q * GROUP, GROUP)].reshape(rows, hidden).astype(F32) * loss_scale
            dh_v[span(q), :] = (gate * dy).astype(BF16)
            big[span(q), :] = jnp.zeros((rows, hidden), F32)

        @pl.loop(0, tiles)
        def _(t):
            step = l * tiles + t
            at = pl.ds(pl.multiple_of(t * TILE, TILE), TILE)

            @pl.loop(0, stages)
            def _(q):
                up = w1_v[l, :, at]
                a = dot(xr_in[0, pl.ds(q * GROUP, GROUP)].reshape(rows, hidden), up)
                th = jnp.tanh(C0 * (a + C1 * (a * a * a)))
                side = 0.5 * (1.0 + th)
                u_t[span(q), :] = (a * side).astype(BF16)
                slope = side + 0.5 * a * (1.0 - th * th) * (C0 + (3.0 * C0 * C1) * (a * a))
                du = dot(dh_v[span(q), :], w2_v[l, at, :], 1, 1).astype(BF16).astype(F32)
                da = (slope * du).astype(BF16)
                da_t[span(q), :] = da
                big[span(q), :] += dot(da, up, 1, 1)

            @pl.when(step > 0)
            def _():
                grads_out(step - 1)

            @pl.loop(0, TILE // rows)
            def _(m):
                part = dot(u_t[:, span(m)], dh_v[...], 0, 0).astype(BF16)
                w2_v[l, pl.ds(pl.multiple_of(t * TILE + m * rows, rows), rows), :] = part

            @pl.loop(0, hidden // rows)
            def _(m):
                xm = xr_in[0, :, :, span(m)].reshape(tok, rows)
                w1_v[l, span(m), at] = dot(xm, da_t[...], 0, 0).astype(BF16)

        @pl.loop(0, stages)
        def _(q):
            gs[l, pl.ds(q * GROUP, GROUP)] = big[span(q), :].astype(BF16).reshape(GROUP, per, hidden)

        @pl.when(l < local_experts - 1)
        def _():
            @pl.loop(0, stages)
            def _(i):
                send_g(l, i, 0, GROUP)
    grads_out(local_experts * tiles - 1)

    all_h = remote(hs.at[most], h_in.at[most], h_ss, h_rs, me)
    all_h.wait_recv()

    @pl.loop(0, stages)
    def _(q):
        big[span(q), :] = xr_v[0, span(q), :].astype(F32)
        d_acc[span(q), :] = jnp.zeros((rows, 3 * experts), F32)

    @pl.loop(0, stages)
    def _(q):
        blocks = pl.ds(q * GROUP, GROUP)
        slot_probs = softmax(dot(xr_s[0, blocks].reshape(rows, hidden), wg[...], 1, 1))
        dy = xr_s[1, blocks].reshape(rows, hidden).astype(F32) * loss_scale
        mixed, d_slot = 0.0, 0.0
        for l in range(local_experts):
            here = lane_e == (q * GROUP + row_dev) * local_experts + l
            h = h_in[blocks, l * per:(l + 1) * per, :].reshape(rows, hidden).astype(F32)
            mixed += jnp.sum(jnp.where(here, slot_probs, 0.0), axis=1, keepdims=True) * h
            d_slot += jnp.where(here, jnp.sum(dy * h, axis=1, keepdims=True), 0.0)
        m3 = jnp.concatenate(split3(mixed), axis=0)
        d3 = jnp.concatenate(split3(d_slot), axis=1)

        @pl.loop(0, stages)
        def _(c):
            p = pick[span(q), span(c)]
            big[span(c), :] += dot(jnp.concatenate([p, p, p], axis=0), m3, 0, 0)
            d_acc[span(c), :] += dot(p, d3, 0, 0)

    acc[pl.ds(0, 8), pl.ds(0, LANES)] = jnp.zeros((8, LANES), F32)
    big_g = acc.at[pl.ds(64, experts), :]
    big_g[...] = jnp.zeros((experts, hidden), F32)

    @pl.loop(0, stages)
    def _(c):
        y = big[span(c), :].astype(BF16)
        out_st[span(c), :] = y
        lost = jnp.sum(y.astype(F32) * xr_v[1, span(c), :].astype(F32), axis=0, keepdims=True)
        acc[pl.ds(0, 1), pl.ds(0, LANES)] += jnp.broadcast_to(jnp.sum(lost, axis=1, keepdims=True), (1, LANES))
        d3 = d_acc[span(c), :]
        d_probs = d3[:, :experts] + d3[:, experts:2 * experts] + d3[:, 2 * experts:]
        probs = s_own[span(c), :]
        dl = (probs * (d_probs - jnp.sum(probs * d_probs, axis=1, keepdims=True))).astype(BF16)
        dlog[span(c), :] = dl
        big_g[...] += dot(dl, xr_v[0, span(c), :], 0, 0)
    y_dma = pltpu.make_async_copy(out_st, y_out, out_sem.at[2])

    wide = hidden // 2
    lost = jnp.broadcast_to(acc[pl.ds(0, 1), pl.ds(0, LANES)], (8, LANES)) * loss_scale
    for c in range(half):
        red_s[c, :, :wide] = big_g[8 * (c // 2):8 * (c // 2) + 8, wide * (c % 2):wide * (c % 2) + wide]
        red_s[c, :, wide:] = lost
    mine = me % half
    red_in[mine] = red_s[mine]

    @pl.loop(0, stages)
    def _(c):
        big[span(c), :] = xr_v[1, span(c), :].astype(F32) * loss_scale + dot(dlog[span(c), :], wg[...], 1, 0)
    y_dma.start()

    @pl.loop(half, n - 1)
    def _(p):
        d = peer(p)
        remote(red_s.at[d % half], red_in.at[mine], red_ss, red_rs, d).start()
    send_g(local_experts - 1, 0, 0, GROUP)

    def add_g(l, i):
        await_group(lambda b: g_in.at[l, b], g_rs.at[l * stages + i], i)
        q = group(i)
        g = g_in[l, pl.ds(q * GROUP, GROUP)].reshape(rows, hidden)

        @pl.loop(0, stages)
        def _(c):
            big[span(c), :] += dot(pick[span(q), span(c)], g, 0, 0)

    @pl.loop(0, (local_experts - 1) * stages)
    def _(s):
        add_g(s // stages, s % stages)

    some = pl.ds(0, half - 1)
    red = remote(red_s.at[some], red_in.at[some], red_ss, red_rs, me)
    red.wait_recv()
    swap_s[...] = jnp.sum(red_in[...], axis=0)
    last = local_experts - 1

    @pl.loop(2, stages)
    def _(i):
        send_g(last, i, 0, GROUP)
    swap = remote(swap_s, swap_in, swap_ss, swap_rs, peer(half - 1))
    swap.start()
    send_g(last, 1, 0, GROUP // 2)
    swap.wait_recv()
    full = swap_s[...] + swap_in[...]
    loss_out[...] = full[:, wide:]
    all_s[...] = full[:, :wide]
    all_in[mine] = full[:, :wide]

    @pl.loop(2, stages)
    def _(i):
        add_g(last, i)

    @pl.loop(half, n - 1)
    def _(p):
        remote(all_s, all_in.at[mine], all_ss, all_rs, peer(p)).start()
    send_g(last, 1, GROUP // 2, GROUP)
    add_g(last, 0)
    gathered = remote(all_in.at[some], all_in.at[some], all_ss, all_rs, me)
    gathered.wait_recv()
    for c in range(half):
        gg_out[8 * (c // 2):8 * (c // 2) + 8, wide * (c % 2):wide * (c % 2) + wide] = all_in[c]
    y_dma.wait()
    add_g(last, 1)

    @pl.loop(0, stages)
    def _(c):
        out_st[span(c), :] = big[span(c), :].astype(BF16)
    gx_dma = pltpu.make_async_copy(out_st, gx_out, out_sem.at[3])
    swap.wait_send()
    red.wait_send()
    gathered.wait_send()
    all_h.wait_send()
    for w in range(2):
        remote(xr_s.at[w, most], xr_in.at[w, most], xr_ss, xr_rs.at[0], me).wait_send()
    for l in range(local_experts):
        remote(gs.at[l, most], g_in.at[l, most], g_ss, g_rs.at[0], me).wait_send()
    gx_dma.start()
    pltpu.make_async_copy(w1_v, gu_out, out_sem.at[0]).wait()
    pltpu.make_async_copy(w2_v, gd_out, out_sem.at[1]).wait()
    gx_dma.wait()


def solution(mesh):
    n = mesh.shape['ep']

    def device_step(x, gate_w, up_w, down_w, expert_picks, loss_w):
        tok, hidden = x.shape
        local_experts, capacity = expert_picks.shape
        per = capacity // n
        experts = gate_w.shape[1]
        loss_scale = 1.0 / math.sqrt(tok * n * hidden)
        rows = GROUP * per
        half = n // 2
        hbm = pl.BlockSpec(memory_space=pl.ANY)
        vmem = pl.BlockSpec(memory_space=pltpu.VMEM)
        dma = pltpu.SemaphoreType.DMA
        blocks = (n, per, hidden)
        wide = (n, local_experts * per, hidden)
        chunk = (8, hidden // 2)
        flat = jax.ShapeDtypeStruct(x.shape, BF16)
        y, grad_x, grad_up, grad_down, grad_gate, loss = pl.pallas_call(
            functools.partial(moe_kernel, n, loss_scale),
            out_shape=[flat, flat, jax.ShapeDtypeStruct(up_w.shape, BF16), jax.ShapeDtypeStruct(down_w.shape, BF16),
                       jax.ShapeDtypeStruct((experts, hidden), F32), jax.ShapeDtypeStruct((8, LANES), F32)],
            in_specs=[vmem, hbm, hbm, vmem, hbm, hbm],
            out_specs=[hbm] * 4 + [vmem] * 2,
            scratch_shapes=[
                pltpu.VMEM((2, tok, hidden), BF16), pltpu.VMEM(up_w.shape, BF16), pltpu.VMEM(down_w.shape, BF16),
                pltpu.VMEM((capacity, tok), BF16), pltpu.VMEM((2,) + blocks, BF16), pltpu.VMEM((2,) + blocks, BF16),
                pltpu.VMEM(wide, BF16), pltpu.VMEM(wide, BF16),
                pltpu.VMEM((local_experts,) + blocks, BF16), pltpu.VMEM((local_experts,) + blocks, BF16),
                pltpu.VMEM((capacity, hidden), BF16), pltpu.VMEM((capacity, experts), F32), pltpu.VMEM((tok, experts), F32),
                pltpu.VMEM((capacity, TILE), BF16), pltpu.VMEM((capacity, TILE), BF16),
                pltpu.VMEM((rows, hidden), F32), pltpu.VMEM((capacity, hidden), F32), pltpu.VMEM((tok, hidden), BF16),
                pltpu.VMEM((n, 1, LANES), jnp.int32), pltpu.VMEM((LANES, LANES), F32),
                pltpu.VMEM((tok, 3 * experts), F32), pltpu.VMEM((tok, experts), BF16),
                pltpu.VMEM((half, 8, hidden // 2 + LANES), F32), pltpu.VMEM((half, 8, hidden // 2 + LANES), F32),
                pltpu.VMEM((8, hidden // 2 + LANES), F32), pltpu.VMEM((8, hidden // 2 + LANES), F32),
                pltpu.VMEM(chunk, F32), pltpu.VMEM((half,) + chunk, F32),
                dma((4,)), dma, dma, dma, dma((2 * n // GROUP,)), dma, dma, dma, dma((local_experts * n // GROUP,)),
                dma, dma, dma, dma, dma, dma, dma((4,))],
            compiler_params=pltpu.CompilerParams(collective_id=0, has_side_effects=True, vmem_limit_bytes=63 * 1024 * 1024),
            name='moe',
        )(expert_picks[0].reshape(-1, 1, LANES), x, loss_w, gate_w.T, up_w, down_w)
        return y, loss[0, 0], grad_x, grad_up, grad_down, grad_gate.T

    return jax.shard_map(device_step, mesh=mesh,
                         in_specs=(P('ep'), P(), P('ep'), P('ep'), P('ep'), P('ep')),
                         out_specs=(P('ep'), P(), P('ep'), P('ep'), P('ep'), P()),
                         check_vma=False)
```

```python
import functools
import math
import jax
import jax.numpy as jnp
from jax import lax
from jax.experimental import pallas as pl
from jax.experimental.pallas import tpu as pltpu
from jax.sharding import PartitionSpec as P

F32 = jnp.float32
BF16 = jnp.bfloat16
GROUP = 8
TILE = 512
LANES = 128
C0 = math.sqrt(2.0 / math.pi)
C1 = 0.044715


def dot(a, b, ca=1, cb=0):
    return lax.dot_general(a, b, (((ca,), (cb,)), ((), ())), preferred_element_type=F32)


def split3(v):
    hi = v.astype(BF16)
    rest = v - hi.astype(F32)
    mid = rest.astype(BF16)
    return hi, mid, (rest - mid.astype(F32)).astype(BF16)


def softmax(logits):
    e = jnp.exp(logits - jnp.max(logits, axis=1, keepdims=True))
    return e / jnp.sum(e, axis=1, keepdims=True)


def xor(a, b, bits):
    return sum(((a // (1 << i) + b // (1 << i)) % 2) * (1 << i) for i in range(bits))


def moe_kernel(n, loss_scale, ids, x, r, wg, w1, w2,
               y_out, gx_out, w1_v, w2_v, gg_out, loss_out, u_far, da_far,
               xr_v, pick, xr_s, xr_in, hs, h_in, gs, g_in, dh_v, s_in, s_own, u_t, da_t, acc, big,
               ids_in, ids_t, d_acc, dlog, red_s, red_in, swap_s, swap_in, all_s, all_in,
               load_sem, ids_ss, ids_rs, xr_ss, xr_rs, h_ss, h_rs, g_ss, g_rs, red_ss, red_rs, swap_ss, swap_rs, all_ss, all_rs, put_sem, get_sem):
    me = lax.axis_index('ep')
    bits = n.bit_length() - 1
    stages = n // GROUP
    half = n // 2
    tok, hidden = xr_v.shape[1:]
    per = tok // n
    rows = GROUP * per
    local_experts, _, ffn = w1_v.shape
    tiles = ffn // TILE
    experts = wg.shape[0]
    most = pl.ds(0, n - 1)

    def peer(p):
        return xor(me, n - 1 - p, bits)

    def group(i):
        return xor(me // GROUP, stages - 1 - i, bits - 3)

    def remote(src, dst, ss, rs, d):
        return pltpu.make_async_remote_copy(src, dst, ss, rs, device_id=(d,), device_id_type=pl.DeviceIdType.MESH)

    def span(q):
        return pl.ds(pl.multiple_of(q * rows, rows), rows)

    loads = [pltpu.make_async_copy(x, xr_v.at[0], load_sem.at[0]), pltpu.make_async_copy(r, xr_v.at[1], load_sem.at[1]),
             pltpu.make_async_copy(w1, w1_v, load_sem.at[2]), pltpu.make_async_copy(w2, w2_v, load_sem.at[3])]
    for c in loads:
        c.start()

    barrier = pltpu.get_barrier_semaphore()

    @pl.loop(0, n - 1)
    def _(p):
        pl.semaphore_signal(barrier, inc=1, device_id=(peer(p),), device_id_type=pl.DeviceIdType.MESH)
    pl.semaphore_wait(barrier, n - 1)

    packed = LANES // per

    @pl.loop(0, n - 1)
    def _(p):
        d = peer(p)
        remote(ids.at[d // packed], ids_in.at[me], ids_ss, ids_rs, d).start()
    ids_in[me] = ids[me // packed]
    all_ids = remote(ids_in.at[most], ids_in.at[most], ids_ss, ids_rs, me)
    all_ids.wait_send()
    all_ids.wait_recv()
    flat = ids_in[...].reshape(n, LANES).astype(F32)
    ids_t[...] = jnp.transpose(jnp.concatenate([flat] * (LANES // n), axis=0))
    cols = ids_t[pl.ds(pl.multiple_of((me % packed) * per, per), per), :]
    lane = lax.broadcasted_iota(jnp.int32, (per, LANES), 1)
    tok_iota = (lax.broadcasted_iota(jnp.int32, (per, tok), 1) + me * tok).astype(F32)

    loads[0].wait()
    loads[1].wait()

    @pl.loop(0, 2 * stages + 1)
    def _(s):
        @pl.when(s < stages)
        def _():
            base = group(s % stages) * GROUP
            for j in range(GROUP):
                col = jnp.sum(jnp.where(lane == base + j, cols, 0.0), axis=1, keepdims=True)
                at = pl.multiple_of((base + j) * per, per)
                pick[pl.ds(at, per), :] = jnp.where(tok_iota == col, 1.0, 0.0).astype(BF16)

        @pl.when(s < 2 * stages)
        def _():
            w, q = s // stages, group(s % stages)
            xr_s[w, pl.ds(q * GROUP, GROUP)] = dot(pick[span(q), :], xr_v[w]).astype(BF16).reshape(GROUP, per, hidden)

        @pl.when(s > 0)
        def _():
            w, i = (s - 1) // stages, (s - 1) % stages

            @pl.loop(0, GROUP)
            def _(j):
                p = i * GROUP + j

                @pl.when(p < n - 1)
                def _():
                    d = peer(p)
                    remote(xr_s.at[w, d], xr_in.at[w, me], xr_ss, xr_rs.at[w * stages + i], d).start()

                @pl.when(p == n - 1)
                def _():
                    xr_in[w, me] = xr_s[w, me]

    @pl.loop(0, stages)
    def _(c):
        s_own[span(c), :] = softmax(dot(xr_v[0, span(c), :], wg[...], 1, 1))
    loads[2].wait()
    loads[3].wait()

    def await_group(ref, sem, i):
        for cond, size in ((i < stages - 1, GROUP), (i == stages - 1, GROUP - 1)):
            @pl.when(cond)
            def _():
                part = ref(pl.ds(group(i) * GROUP, size))
                remote(part, part, xr_ss, sem, me).wait_recv()

    def send_h(i):
        @pl.loop(0, GROUP)
        def _(j):
            p = i * GROUP + j

            @pl.when(p < n - 1)
            def _():
                d = peer(p)
                remote(hs.at[d], h_in.at[me], h_ss, h_rs, d).start()

            @pl.when(p == n - 1)
            def _():
                h_in[me] = hs[me]

    lane_e = lax.broadcasted_iota(jnp.int32, (rows, experts), 1)
    row_dev = lax.broadcasted_iota(jnp.int32, (rows, experts), 0) // per

    @pl.loop(0, stages)
    def _(i):
        q = group(i)
        await_group(lambda b: xr_in.at[0, b], xr_rs.at[i], i)
        xg = xr_in[0, pl.ds(q * GROUP, GROUP)].reshape(rows, hidden)
        s_in[span(q), :] = softmax(dot(xg, wg[...], 1, 1))

        @pl.when(i > 0)
        def _():
            send_h(i - 1)

        @pl.loop(0, local_experts)
        def _(l):
            acc[...] = jnp.zeros_like(acc)

            @pl.loop(0, tiles, unroll=2)
            def _(t):
                at = pl.ds(pl.multiple_of(t * TILE, TILE), TILE)
                a = dot(xg, w1_v[l, :, at])
                u = (0.5 * a * (1.0 + jnp.tanh(C0 * (a + C1 * (a * a * a))))).astype(BF16)
                acc[...] += dot(u, w2_v[l, at, :])
            hs[pl.ds(q * GROUP, GROUP), pl.ds(pl.multiple_of(l * per, per), per), :] = acc[...].astype(BF16).reshape(GROUP, per, hidden)

    @pl.loop(0, stages)
    def _(i):
        await_group(lambda b: xr_in.at[1, b], xr_rs.at[stages + i], i)

        @pl.when(i == 0)
        def _():
            send_h(stages - 1)

    def wide_of(l):
        return pl.ds(pl.multiple_of(l * per, per), per)

    def send_g(l, i, lo, hi):
        @pl.loop(lo, hi)
        def _(j):
            p = i * GROUP + j

            @pl.when(p < n - 1)
            def _():
                d = peer(p)
                remote(gs.at[l, d], g_in.at[l, me], g_ss, g_rs.at[l * stages + i], d).start()

            @pl.when(p == n - 1)
            def _():
                g_in[l, me] = gs[l, me]

    def tile_at(t):
        return pl.ds(pl.multiple_of(t * TILE, TILE), TILE)

    def start_rows(l):
        @pl.loop(0, stages)
        def _(q):
            gate = jnp.sum(jnp.where(lane_e == me * local_experts + l, s_in[span(q), :], 0.0), axis=1, keepdims=True)
            dy = xr_in[1, pl.ds(q * GROUP, GROUP)].reshape(rows, hidden).astype(F32) * loss_scale
            dh_v[span(q), :] = (gate * dy).astype(BF16)
            big[span(q), :] = jnp.zeros((rows, hidden), F32)

    def row_grads(l, t, slot):
        at = tile_at(t)

        @pl.loop(0, stages, unroll=2)
        def _(q):
            up = w1_v[l, :, at]
            a = dot(xr_in[0, pl.ds(q * GROUP, GROUP)].reshape(rows, hidden), up)
            th = jnp.tanh(C0 * (a + C1 * (a * a * a)))
            side = 0.5 * (1.0 + th)
            u_t[slot, span(q), :] = (a * side).astype(BF16)
            slope = side + 0.5 * a * (1.0 - th * th) * (C0 + (3.0 * C0 * C1) * (a * a))
            du = dot(dh_v[span(q), :], w2_v[l, at, :], 1, 1).astype(BF16).astype(F32)
            da = (slope * du).astype(BF16)
            da_t[slot, span(q), :] = da
            big[span(q), :] += dot(da, up, 1, 1)

    def weight_grads(l, t, slot):
        at = tile_at(t)

        @pl.loop(0, TILE // rows)
        def _(m):
            part = dot(u_t[slot, :, span(m)], dh_v[...], 0, 0).astype(BF16)
            w2_v[l, pl.ds(pl.multiple_of(t * TILE + m * rows, rows), rows), :] = part

        @pl.loop(0, hidden // rows)
        def _(m):
            xm = xr_in[0, :, :, span(m)].reshape(tok, rows)
            w1_v[l, span(m), at] = dot(xm, da_t[slot], 0, 0).astype(BF16)

    def finish_rows(l):
        @pl.loop(0, stages)
        def _(q):
            gs[l, pl.ds(q * GROUP, GROUP)] = big[span(q), :].astype(BF16).reshape(GROUP, per, hidden)

    last = local_experts - 1

    @pl.loop(0, last)
    def _(l):
        start_rows(l)

        @pl.loop(0, tiles)
        def _(t):
            row_grads(l, t, 0)
            weight_grads(l, t, 0)
        finish_rows(l)

        @pl.loop(0, stages)
        def _(i):
            send_g(l, i, 0, GROUP)

    def aside(t, slot):
        return (pltpu.make_async_copy(u_t.at[slot], u_far.at[t], put_sem.at[slot]),
                pltpu.make_async_copy(da_t.at[slot], da_far.at[t], put_sem.at[2 + slot]))

    def fetch(t, slot):
        return (pltpu.make_async_copy(u_far.at[t], u_t.at[slot], get_sem.at[slot]),
                pltpu.make_async_copy(da_far.at[t], da_t.at[slot], get_sem.at[2 + slot]))

    start_rows(last)

    @pl.loop(0, tiles)
    def _(t):
        slot = t % 2

        @pl.when(t >= 2)
        def _():
            for c in aside(t - 2, slot):
                c.wait()
        row_grads(last, t, slot)

        @pl.when(t < tiles - 2)
        def _():
            for c in aside(t, slot):
                c.start()
    finish_rows(last)
    for slot in range(2):
        weight_grads(last, tiles - 2 + slot, slot)
        for c in fetch(slot, slot):
            c.start()

    all_h = remote(hs.at[most], h_in.at[most], h_ss, h_rs, me)
    all_h.wait_recv()

    @pl.loop(0, stages)
    def _(q):
        big[span(q), :] = xr_v[0, span(q), :].astype(F32)
        d_acc[span(q), :] = jnp.zeros((rows, 3 * experts), F32)

    @pl.loop(0, stages)
    def _(q):
        blocks = pl.ds(q * GROUP, GROUP)
        slot_probs = softmax(dot(xr_s[0, blocks].reshape(rows, hidden), wg[...], 1, 1))
        dy = xr_s[1, blocks].reshape(rows, hidden).astype(F32) * loss_scale
        mixed, d_slot = 0.0, 0.0
        for l in range(local_experts):
            here = lane_e == (q * GROUP + row_dev) * local_experts + l
            h = h_in[blocks, l * per:(l + 1) * per, :].reshape(rows, hidden).astype(F32)
            mixed += jnp.sum(jnp.where(here, slot_probs, 0.0), axis=1, keepdims=True) * h
            d_slot += jnp.where(here, jnp.sum(dy * h, axis=1, keepdims=True), 0.0)
        m3 = jnp.concatenate(split3(mixed), axis=0)
        d3 = jnp.concatenate(split3(d_slot), axis=1)

        @pl.loop(0, stages)
        def _(c):
            p = pick[span(q), span(c)]
            big[span(c), :] += dot(jnp.concatenate([p, p, p], axis=0), m3, 0, 0)
            d_acc[span(c), :] += dot(p, d3, 0, 0)

    acc[pl.ds(0, 8), pl.ds(0, LANES)] = jnp.zeros((8, LANES), F32)
    big_g = acc.at[pl.ds(64, experts), :]
    big_g[...] = jnp.zeros((experts, hidden), F32)

    @pl.loop(0, stages)
    def _(c):
        y = big[span(c), :].astype(BF16)
        y_out[span(c), :] = y
        lost = jnp.sum(y.astype(F32) * xr_v[1, span(c), :].astype(F32), axis=0, keepdims=True)
        acc[pl.ds(0, 1), pl.ds(0, LANES)] += jnp.broadcast_to(jnp.sum(lost, axis=1, keepdims=True), (1, LANES))
        d3 = d_acc[span(c), :]
        d_probs = d3[:, :experts] + d3[:, experts:2 * experts] + d3[:, 2 * experts:]
        probs = s_own[span(c), :]
        dl = (probs * (d_probs - jnp.sum(probs * d_probs, axis=1, keepdims=True))).astype(BF16)
        dlog[span(c), :] = dl
        big_g[...] += dot(dl, xr_v[0, span(c), :], 0, 0)

    wide = hidden // 2
    lost = jnp.broadcast_to(acc[pl.ds(0, 1), pl.ds(0, LANES)], (8, LANES)) * loss_scale
    for c in range(half):
        red_s[c, :, :wide] = big_g[8 * (c // 2):8 * (c // 2) + 8, wide * (c % 2):wide * (c % 2) + wide]
        red_s[c, :, wide:] = lost
    mine = me % half
    red_in[mine] = red_s[mine]

    @pl.loop(0, stages)
    def _(c):
        big[span(c), :] = xr_v[1, span(c), :].astype(F32) * loss_scale + dot(dlog[span(c), :], wg[...], 1, 0)

    @pl.loop(half, n - 1)
    def _(p):
        d = peer(p)
        remote(red_s.at[d % half], red_in.at[mine], red_ss, red_rs, d).start()
    @pl.loop(2, stages)
    def _(i):
        send_g(last, i, 0, GROUP)
    send_g(last, 0, 0, GROUP)

    @pl.loop(0, tiles - 2)
    def _(t):
        slot = t % 2
        for c in fetch(t, slot):
            c.wait()
        weight_grads(last, t, slot)

        @pl.when(t < tiles - 4)
        def _():
            for c in fetch(t + 2, slot):
                c.start()

    def add_g(l, i):
        await_group(lambda b: g_in.at[l, b], g_rs.at[l * stages + i], i)
        q = group(i)
        g = g_in[l, pl.ds(q * GROUP, GROUP)].reshape(rows, hidden)

        @pl.loop(0, stages)
        def _(c):
            big[span(c), :] += dot(pick[span(q), span(c)], g, 0, 0)

    @pl.loop(0, last * stages - 1)
    def _(s):
        add_g(s // stages, s % stages)

    some = pl.ds(0, half - 1)
    red = remote(red_s.at[some], red_in.at[some], red_ss, red_rs, me)
    red.wait_recv()
    swap_s[...] = jnp.sum(red_in[...], axis=0)
    add_g(last - 1, stages - 1)
    swap = remote(swap_s, swap_in, swap_ss, swap_rs, peer(half - 1))
    swap.start()
    send_g(last, 1, 0, GROUP)
    add_g(last, 2)
    swap.wait_recv()
    full = swap_s[...] + swap_in[...]
    loss_out[...] = full[:, wide:]
    all_s[...] = full[:, :wide]
    all_in[mine] = full[:, :wide]
    add_g(last, 3)

    @pl.loop(half, n - 1)
    def _(p):
        remote(all_s, all_in.at[mine], all_ss, all_rs, peer(p)).start()
    add_g(last, 0)
    add_g(last, 1)

    @pl.loop(0, stages)
    def _(c):
        gx_out[span(c), :] = big[span(c), :].astype(BF16)
    gathered = remote(all_in.at[some], all_in.at[some], all_ss, all_rs, me)
    gathered.wait_recv()
    for c in range(half):
        gg_out[8 * (c // 2):8 * (c // 2) + 8, wide * (c % 2):wide * (c % 2) + wide] = all_in[c]
    swap.wait_send()
    red.wait_send()
    gathered.wait_send()
    all_h.wait_send()
    for w in range(2):
        remote(xr_s.at[w, most], xr_in.at[w, most], xr_ss, xr_rs.at[0], me).wait_send()
    for l in range(local_experts):
        remote(gs.at[l, most], g_in.at[l, most], g_ss, g_rs.at[0], me).wait_send()


def solution(mesh):
    n = mesh.shape['ep']

    def device_step(x, gate_w, up_w, down_w, expert_picks, loss_w):
        tok, hidden = x.shape
        local_experts, capacity = expert_picks.shape
        per = capacity // n
        experts = gate_w.shape[1]
        loss_scale = 1.0 / math.sqrt(tok * n * hidden)
        rows = GROUP * per
        half = n // 2
        hbm = pl.BlockSpec(memory_space=pl.ANY)
        vmem = pl.BlockSpec(memory_space=pltpu.VMEM)
        dma = pltpu.SemaphoreType.DMA
        blocks = (n, per, hidden)
        wide = (n, local_experts * per, hidden)
        chunk = (8, hidden // 2)
        flat = pltpu.VMEM(x.shape, BF16)
        aside = jax.ShapeDtypeStruct((up_w.shape[2] // TILE, capacity, TILE), BF16)
        y, grad_x, grad_up, grad_down, grad_gate, loss, _, _ = pl.pallas_call(
            functools.partial(moe_kernel, n, loss_scale),
            out_shape=[flat, flat, pltpu.VMEM(up_w.shape, BF16), pltpu.VMEM(down_w.shape, BF16),
                       jax.ShapeDtypeStruct((experts, hidden), F32), jax.ShapeDtypeStruct((8, LANES), F32)] + [aside] * 2,
            in_specs=[vmem, hbm, hbm, vmem, hbm, hbm],
            out_specs=[vmem] * 6 + [hbm] * 2,
            scratch_shapes=[
                pltpu.VMEM((2, tok, hidden), BF16),
                pltpu.VMEM((capacity, tok), BF16), pltpu.VMEM((2,) + blocks, BF16), pltpu.VMEM((2,) + blocks, BF16),
                pltpu.VMEM(wide, BF16), pltpu.VMEM(wide, BF16),
                pltpu.VMEM((local_experts,) + blocks, BF16), pltpu.VMEM((local_experts,) + blocks, BF16),
                pltpu.VMEM((capacity, hidden), BF16), pltpu.VMEM((capacity, experts), F32), pltpu.VMEM((tok, experts), F32),
                pltpu.VMEM((2, capacity, TILE), BF16), pltpu.VMEM((2, capacity, TILE), BF16),
                pltpu.VMEM((rows, hidden), F32), pltpu.VMEM((capacity, hidden), F32),
                pltpu.VMEM((n, 1, LANES), jnp.int32), pltpu.VMEM((LANES, LANES), F32),
                pltpu.VMEM((tok, 3 * experts), F32), pltpu.VMEM((tok, experts), BF16),
                pltpu.VMEM((half, 8, hidden // 2 + LANES), F32), pltpu.VMEM((half, 8, hidden // 2 + LANES), F32),
                pltpu.VMEM((8, hidden // 2 + LANES), F32), pltpu.VMEM((8, hidden // 2 + LANES), F32),
                pltpu.VMEM(chunk, F32), pltpu.VMEM((half,) + chunk, F32),
                dma((4,)), dma, dma, dma, dma((2 * n // GROUP,)), dma, dma, dma, dma((local_experts * n // GROUP,)),
                dma, dma, dma, dma, dma, dma, dma((4,)), dma((4,))],
            compiler_params=pltpu.CompilerParams(collective_id=0, has_side_effects=True, vmem_limit_bytes=41 * 1024 * 1024),
            name='moe',
        )(expert_picks[0].reshape(-1, 1, LANES), x, loss_w, gate_w.T, up_w, down_w)
        return y, loss[0, 0], grad_x, grad_up, grad_down, grad_gate.T

    return jax.shard_map(device_step, mesh=mesh,
                         in_specs=(P('ep'), P(), P('ep'), P('ep'), P('ep'), P('ep')),
                         out_specs=(P('ep'), P(), P('ep'), P('ep'), P('ep'), P()),
                         check_vma=False)
```

```python
import functools
import math
import jax
import jax.numpy as jnp
from jax import lax
from jax.experimental import pallas as pl
from jax.experimental.pallas import tpu as pltpu
from jax.sharding import PartitionSpec as P

F32 = jnp.float32
BF16 = jnp.bfloat16
GROUP = 8
TILE = 512
LANES = 128
C0 = math.sqrt(2.0 / math.pi)
C1 = 0.044715


def dot(a, b, ca=1, cb=0):
    return lax.dot_general(a, b, (((ca,), (cb,)), ((), ())), preferred_element_type=F32)


def split3(v):
    hi = v.astype(BF16)
    rest = v - hi.astype(F32)
    mid = rest.astype(BF16)
    return hi, mid, (rest - mid.astype(F32)).astype(BF16)


def softmax(logits):
    e = jnp.exp(logits - jnp.max(logits, axis=1, keepdims=True))
    return e / jnp.sum(e, axis=1, keepdims=True)


def xor(a, b, bits):
    return sum(((a // (1 << i) + b // (1 << i)) % 2) * (1 << i) for i in range(bits))


def moe_kernel(n, loss_scale, picks, x, r, gate_w, w1, w2,
               y_out, gx_out, w1_v, w2_v, gg_out, loss_out, u_far, da_far,
               picks_v, ids, wg, xr_v, pick, xr_s, xr_in, hs, h_in, gs, g_in, dh_v, s_in, s_own, u_t, da_t, acc, big,
               ids_in, ids_t, d_acc, dlog, red_s, red_in, swap_s, swap_in, all_s, all_in,
               load_sem, ids_ss, ids_rs, xr_ss, xr_rs, h_ss, h_rs, g_ss, g_rs, red_ss, red_rs, swap_ss, swap_rs, all_ss, all_rs, put_sem, get_sem):
    me = lax.axis_index('ep')
    bits = n.bit_length() - 1
    stages = n // GROUP
    half = n // 2
    tok, hidden = xr_v.shape[1:]
    per = tok // n
    rows = GROUP * per
    local_experts, _, ffn = w1_v.shape
    tiles = ffn // TILE
    experts = wg.shape[0]
    packed = LANES // per
    most = pl.ds(0, n - 1)

    def peer(p):
        return xor(me, n - 1 - p, bits)

    def group(i):
        return xor(me // GROUP, stages - 1 - i, bits - 3)

    def remote(src, dst, ss, rs, d):
        return pltpu.make_async_remote_copy(src, dst, ss, rs, device_id=(d,), device_id_type=pl.DeviceIdType.MESH)

    def span(q):
        return pl.ds(pl.multiple_of(q * rows, rows), rows)

    loads = [pltpu.make_async_copy(picks, picks_v, load_sem.at[4]), pltpu.make_async_copy(gate_w, wg, load_sem.at[5]),
             pltpu.make_async_copy(x, xr_v.at[0], load_sem.at[0]), pltpu.make_async_copy(r, xr_v.at[1], load_sem.at[1]),
             pltpu.make_async_copy(w1, w1_v, load_sem.at[2]), pltpu.make_async_copy(w2, w2_v, load_sem.at[3])]
    for c in loads:
        c.start()

    barrier = pltpu.get_barrier_semaphore()

    @pl.loop(0, n - 1)
    def _(p):
        pl.semaphore_signal(barrier, inc=1, device_id=(peer(p),), device_id_type=pl.DeviceIdType.MESH)

    loads[0].wait()
    for c in range(n // packed):
        ids[c] = picks_v[0:1, c * LANES:(c + 1) * LANES]
    pl.semaphore_wait(barrier, n - 1)

    @pl.loop(0, n - 1)
    def _(p):
        d = peer(p)
        remote(ids.at[d // packed], ids_in.at[me], ids_ss, ids_rs, d).start()
    ids_in[me] = ids[me // packed]
    all_ids = remote(ids_in.at[most], ids_in.at[most], ids_ss, ids_rs, me)
    all_ids.wait_send()
    all_ids.wait_recv()
    flat = ids_in[...].reshape(n, LANES).astype(F32)
    ids_t[...] = jnp.transpose(jnp.concatenate([flat] * (LANES // n), axis=0))
    cols = ids_t[pl.ds(pl.multiple_of((me % packed) * per, per), per), :]
    lane = lax.broadcasted_iota(jnp.int32, (per, LANES), 1)
    tok_iota = (lax.broadcasted_iota(jnp.int32, (per, tok), 1) + me * tok).astype(F32)

    for c in loads[1:4]:
        c.wait()

    def send_rows(s):
        w, i = s // stages, s % stages

        @pl.loop(0, GROUP)
        def _(j):
            p = i * GROUP + j

            @pl.when(p < n - 1)
            def _():
                d = peer(p)
                remote(xr_s.at[w, d], xr_in.at[w, me], xr_ss, xr_rs.at[s], d).start()

            @pl.when(p == n - 1)
            def _():
                xr_in[w, me] = xr_s[w, me]

    def gather_rows(s):
        w, q = s // stages, group(s % stages)
        xr_s[w, pl.ds(q * GROUP, GROUP)] = dot(pick[span(q), :], xr_v[w]).astype(BF16).reshape(GROUP, per, hidden)

    @pl.loop(0, stages)
    def _(s):
        base = group(s) * GROUP
        for j in range(GROUP):
            col = jnp.sum(jnp.where(lane == base + j, cols, 0.0), axis=1, keepdims=True)
            at = pl.multiple_of((base + j) * per, per)
            pick[pl.ds(at, per), :] = jnp.where(tok_iota == col, 1.0, 0.0).astype(BF16)

        @pl.when(s > 0)
        def _():
            send_rows(s - 1)
        gather_rows(s)

    @pl.loop(stages, 2 * stages)
    def _(s):
        gather_rows(s)
        send_rows(s - 1)

    @pl.loop(0, stages)
    def _(c):
        s_own[span(c), :] = softmax(dot(xr_v[0, span(c), :], wg[...], 1, 1))
    send_rows(2 * stages - 1)
    loads[4].wait()
    loads[5].wait()

    @pl.loop(0, stages * stages)
    def _(k):
        q, c = k // stages, k % stages

        @pl.when(c >= q)
        def _():
            upper = jnp.transpose(pick[span(q), span(c)].astype(F32)).astype(BF16)
            lower = jnp.transpose(pick[span(c), span(q)].astype(F32)).astype(BF16)
            pick[span(q), span(c)] = lower
            pick[span(c), span(q)] = upper

    def await_group(ref, sem, i):
        for cond, size in ((i < stages - 1, GROUP), (i == stages - 1, GROUP - 1)):
            @pl.when(cond)
            def _():
                part = ref(pl.ds(group(i) * GROUP, size))
                remote(part, part, xr_ss, sem, me).wait_recv()

    def send_h(i):
        @pl.loop(0, GROUP)
        def _(j):
            p = i * GROUP + j

            @pl.when(p < n - 1)
            def _():
                d = peer(p)
                remote(hs.at[d], h_in.at[me], h_ss, h_rs, d).start()

            @pl.when(p == n - 1)
            def _():
                h_in[me] = hs[me]

    lane_e = lax.broadcasted_iota(jnp.int32, (rows, experts), 1)
    row_dev = lax.broadcasted_iota(jnp.int32, (rows, experts), 0) // per

    @pl.loop(0, stages)
    def _(i):
        q = group(i)
        await_group(lambda b: xr_in.at[0, b], xr_rs.at[i], i)
        xg = xr_in[0, pl.ds(q * GROUP, GROUP)].reshape(rows, hidden)
        s_in[span(q), :] = softmax(dot(xg, wg[...], 1, 1))

        @pl.when(i > 0)
        def _():
            send_h(i - 1)

        @pl.loop(0, local_experts)
        def _(l):
            acc[...] = jnp.zeros_like(acc)

            @pl.loop(0, tiles, unroll=2)
            def _(t):
                at = pl.ds(pl.multiple_of(t * TILE, TILE), TILE)
                a = dot(xg, w1_v[l, :, at])
                u = (0.5 * a * (1.0 + jnp.tanh(C0 * (a + C1 * (a * a * a))))).astype(BF16)
                acc[...] += dot(u, w2_v[l, at, :])
            hs[pl.ds(q * GROUP, GROUP), pl.ds(pl.multiple_of(l * per, per), per), :] = acc[...].astype(BF16).reshape(GROUP, per, hidden)

    @pl.loop(0, stages)
    def _(i):
        await_group(lambda b: xr_in.at[1, b], xr_rs.at[stages + i], i)

        @pl.when(i == 0)
        def _():
            send_h(stages - 1)

    def wide_of(l):
        return pl.ds(pl.multiple_of(l * per, per), per)

    def send_g(l, i, lo, hi):
        @pl.loop(lo, hi)
        def _(j):
            p = i * GROUP + j

            @pl.when(p < n - 1)
            def _():
                d = peer(p)
                remote(gs.at[l, d], g_in.at[l, me], g_ss, g_rs.at[l * stages + i], d).start()

            @pl.when(p == n - 1)
            def _():
                g_in[l, me] = gs[l, me]

    def tile_at(t):
        return pl.ds(pl.multiple_of(t * TILE, TILE), TILE)

    def start_rows(l):
        @pl.loop(0, stages)
        def _(q):
            gate = jnp.sum(jnp.where(lane_e == me * local_experts + l, s_in[span(q), :], 0.0), axis=1, keepdims=True)
            dy = xr_in[1, pl.ds(q * GROUP, GROUP)].reshape(rows, hidden).astype(F32) * loss_scale
            dh_v[span(q), :] = (gate * dy).astype(BF16)
            big[span(q), :] = jnp.zeros((rows, hidden), F32)

    def row_grads(l, t, slot):
        at = tile_at(t)

        @pl.loop(0, stages, unroll=2)
        def _(q):
            up = w1_v[l, :, at]
            a = dot(xr_in[0, pl.ds(q * GROUP, GROUP)].reshape(rows, hidden), up)
            th = jnp.tanh(C0 * (a + C1 * (a * a * a)))
            side = 0.5 * (1.0 + th)
            u_t[slot, span(q), :] = (a * side).astype(BF16)
            slope = side + 0.5 * a * (1.0 - th * th) * (C0 + (3.0 * C0 * C1) * (a * a))
            du = dot(dh_v[span(q), :], w2_v[l, at, :], 1, 1).astype(BF16).astype(F32)
            da = (slope * du).astype(BF16)
            da_t[slot, span(q), :] = da
            big[span(q), :] += dot(da, up, 1, 1)

    def weight_grads(l, t, slot):
        at = tile_at(t)

        @pl.loop(0, TILE // rows)
        def _(m):
            part = dot(u_t[slot, :, span(m)], dh_v[...], 0, 0).astype(BF16)
            w2_v[l, pl.ds(pl.multiple_of(t * TILE + m * rows, rows), rows), :] = part

        @pl.loop(0, hidden // rows)
        def _(m):
            xm = xr_in[0, :, :, span(m)].reshape(tok, rows)
            w1_v[l, span(m), at] = dot(xm, da_t[slot], 0, 0).astype(BF16)

    def finish_rows(l):
        @pl.loop(0, stages)
        def _(q):
            gs[l, pl.ds(q * GROUP, GROUP)] = big[span(q), :].astype(BF16).reshape(GROUP, per, hidden)

    last = local_experts - 1

    @pl.loop(0, last)
    def _(l):
        start_rows(l)

        @pl.loop(0, tiles)
        def _(t):
            row_grads(l, t, 0)
            weight_grads(l, t, 0)
        finish_rows(l)

        @pl.loop(0, stages)
        def _(i):
            send_g(l, i, 0, GROUP)

    def aside(t, slot):
        return (pltpu.make_async_copy(u_t.at[slot], u_far.at[t], put_sem.at[slot]),
                pltpu.make_async_copy(da_t.at[slot], da_far.at[t], put_sem.at[2 + slot]))

    def fetch(t, slot):
        return (pltpu.make_async_copy(u_far.at[t], u_t.at[slot], get_sem.at[slot]),
                pltpu.make_async_copy(da_far.at[t], da_t.at[slot], get_sem.at[2 + slot]))

    start_rows(last)

    @pl.loop(0, tiles)
    def _(t):
        slot = t % 2

        @pl.when(t >= 2)
        def _():
            for c in aside(t - 2, slot):
                c.wait()
        row_grads(last, t, slot)

        @pl.when(t < tiles - 2)
        def _():
            for c in aside(t, slot):
                c.start()
    finish_rows(last)
    for slot in range(2):
        weight_grads(last, tiles - 2 + slot, slot)
        if slot == 0:
            @pl.loop(2, stages)
            def _(i):
                send_g(last, i, 0, GROUP)
            send_g(last, 0, 0, GROUP)
        for c in fetch(slot, slot):
            c.start()

    all_h = remote(hs.at[most], h_in.at[most], h_ss, h_rs, me)
    all_h.wait_recv()

    @pl.loop(0, stages)
    def _(q):
        big[span(q), :] = xr_v[0, span(q), :].astype(F32)
        d_acc[span(q), :] = jnp.zeros((rows, 3 * experts), F32)

    @pl.loop(0, stages)
    def _(q):
        blocks = pl.ds(q * GROUP, GROUP)
        slot_probs = softmax(dot(xr_s[0, blocks].reshape(rows, hidden), wg[...], 1, 1))
        dy = xr_s[1, blocks].reshape(rows, hidden).astype(F32) * loss_scale
        mixed, d_slot = 0.0, 0.0
        for l in range(local_experts):
            here = lane_e == (q * GROUP + row_dev) * local_experts + l
            h = h_in[blocks, l * per:(l + 1) * per, :].reshape(rows, hidden).astype(F32)
            mixed += jnp.sum(jnp.where(here, slot_probs, 0.0), axis=1, keepdims=True) * h
            d_slot += jnp.where(here, jnp.sum(dy * h, axis=1, keepdims=True), 0.0)
        m3 = jnp.concatenate(split3(mixed), axis=0)
        d3 = jnp.concatenate(split3(d_slot), axis=1)

        @pl.loop(0, stages)
        def _(c):
            p = pick[span(c), span(q)]
            big[span(c), :] += dot(jnp.concatenate([p, p, p], axis=1), m3)
            d_acc[span(c), :] += dot(p, d3)

    acc[pl.ds(0, 8), pl.ds(0, LANES)] = jnp.zeros((8, LANES), F32)
    big_g = acc.at[pl.ds(64, experts), :]
    big_g[...] = jnp.zeros((experts, hidden), F32)

    @pl.loop(0, stages)
    def _(c):
        y = big[span(c), :].astype(BF16)
        y_out[span(c), :] = y
        lost = jnp.sum(y.astype(F32) * xr_v[1, span(c), :].astype(F32), axis=0, keepdims=True)
        acc[pl.ds(0, 1), pl.ds(0, LANES)] += jnp.broadcast_to(jnp.sum(lost, axis=1, keepdims=True), (1, LANES))
        d3 = d_acc[span(c), :]
        d_probs = d3[:, :experts] + d3[:, experts:2 * experts] + d3[:, 2 * experts:]
        probs = s_own[span(c), :]
        dl = (probs * (d_probs - jnp.sum(probs * d_probs, axis=1, keepdims=True))).astype(BF16)
        dlog[span(c), :] = dl
        big_g[...] += dot(dl, xr_v[0, span(c), :], 0, 0)

    wide = hidden // 2
    lost = jnp.broadcast_to(acc[pl.ds(0, 1), pl.ds(0, LANES)], (8, LANES)) * loss_scale
    for c in range(half):
        red_s[c, :, :wide] = big_g[8 * (c // 2):8 * (c // 2) + 8, wide * (c % 2):wide * (c % 2) + wide]
        red_s[c, :, wide:] = lost
    mine = me % half
    red_in[mine] = red_s[mine]

    @pl.loop(0, stages)
    def _(c):
        big[span(c), :] = xr_v[1, span(c), :].astype(F32) * loss_scale + dot(dlog[span(c), :], wg[...], 1, 0)

    @pl.loop(half, n - 1)
    def _(p):
        d = peer(p)
        remote(red_s.at[d % half], red_in.at[mine], red_ss, red_rs, d).start()
    send_g(last, 1, 0, GROUP // 2)

    @pl.loop(0, tiles - 2)
    def _(t):
        slot = t % 2
        for c in fetch(t, slot):
            c.wait()
        weight_grads(last, t, slot)

        @pl.when(t < tiles - 4)
        def _():
            for c in fetch(t + 2, slot):
                c.start()

    def add_g(l, i):
        await_group(lambda b: g_in.at[l, b], g_rs.at[l * stages + i], i)
        q = group(i)
        g = g_in[l, pl.ds(q * GROUP, GROUP)].reshape(rows, hidden)

        @pl.loop(0, stages)
        def _(c):
            big[span(c), :] += dot(pick[span(c), span(q)], g)

    some = pl.ds(0, half - 1)
    red = remote(red_s.at[some], red_in.at[some], red_ss, red_rs, me)
    red.wait_recv()
    swap_s[...] = jnp.sum(red_in[...], axis=0)
    add_g(0, 0)
    swap = remote(swap_s, swap_in, swap_ss, swap_rs, peer(half - 1))
    swap.start()
    send_g(last, 1, GROUP // 2, GROUP)

    @pl.loop(1, last * stages)
    def _(s):
        add_g(s // stages, s % stages)
    add_g(last, 2)
    swap.wait_recv()
    full = swap_s[...] + swap_in[...]
    loss_out[...] = full[:, wide:]
    all_s[...] = full[:, :wide]
    all_in[mine] = full[:, :wide]
    add_g(last, 3)

    @pl.loop(half, n - 1)
    def _(p):
        remote(all_s, all_in.at[mine], all_ss, all_rs, peer(p)).start()
    add_g(last, 0)
    add_g(last, 1)

    @pl.loop(0, stages)
    def _(c):
        gx_out[span(c), :] = big[span(c), :].astype(BF16)
    gathered = remote(all_in.at[some], all_in.at[some], all_ss, all_rs, me)
    gathered.wait_recv()
    for c in range(half):
        gg_out[8 * (c // 2):8 * (c // 2) + 8, wide * (c % 2):wide * (c % 2) + wide] = all_in[c]
    swap.wait_send()
    red.wait_send()
    gathered.wait_send()
    all_h.wait_send()
    for w in range(2):
        remote(xr_s.at[w, most], xr_in.at[w, most], xr_ss, xr_rs.at[0], me).wait_send()
    for l in range(local_experts):
        remote(gs.at[l, most], g_in.at[l, most], g_ss, g_rs.at[0], me).wait_send()


def flush_kernel(y, gx, gu, gd, gg, loss, y_out, gx_out, gu_out, gd_out, gg_out, loss_out, sem):
    parts = [(gu.at[l], gu_out.at[l]) for l in range(gu.shape[0])] + [(gd.at[l], gd_out.at[l]) for l in range(gd.shape[0])]
    parts += [(y, y_out), (gx, gx_out), (gg, gg_out)]
    copies = [pltpu.make_async_copy(a, b, sem.at[k]) for k, (a, b) in enumerate(parts)]
    for c in copies:
        c.start()
    loss_out[0, 0] = loss[0, 0]
    for c in copies:
        c.wait()


def solution(mesh):
    n = mesh.shape['ep']

    def device_step(x, gate_w, up_w, down_w, expert_picks, loss_w):
        tok, hidden = x.shape
        local_experts, capacity = expert_picks.shape
        per = capacity // n
        experts = gate_w.shape[1]
        loss_scale = 1.0 / math.sqrt(tok * n * hidden)
        rows = GROUP * per
        half = n // 2
        hbm = pl.BlockSpec(memory_space=pl.ANY)
        vmem = pl.BlockSpec(memory_space=pltpu.VMEM)
        dma = pltpu.SemaphoreType.DMA
        blocks = (n, per, hidden)
        wide = (n, local_experts * per, hidden)
        chunk = (8, hidden // 2)
        flat = pltpu.VMEM(x.shape, BF16)
        aside = jax.ShapeDtypeStruct((up_w.shape[2] // TILE, capacity, TILE), BF16)
        *held, _, _ = pl.pallas_call(
            functools.partial(moe_kernel, n, loss_scale),
            out_shape=[flat, flat, pltpu.VMEM(up_w.shape, BF16), pltpu.VMEM(down_w.shape, BF16),
                       pltpu.VMEM((experts, hidden), F32), pltpu.VMEM((8, LANES), F32)] + [aside] * 2,
            in_specs=[hbm] * 6,
            out_specs=[vmem] * 6 + [hbm] * 2,
            scratch_shapes=[
                pltpu.VMEM(expert_picks.shape, jnp.int32), pltpu.VMEM((capacity // LANES, 1, LANES), jnp.int32),
                pltpu.VMEM((experts, hidden), BF16), pltpu.VMEM((2, tok, hidden), BF16),
                pltpu.VMEM((capacity, tok), BF16), pltpu.VMEM((2,) + blocks, BF16), pltpu.VMEM((2,) + blocks, BF16),
                pltpu.VMEM(wide, BF16), pltpu.VMEM(wide, BF16),
                pltpu.VMEM((local_experts,) + blocks, BF16), pltpu.VMEM((local_experts,) + blocks, BF16),
                pltpu.VMEM((capacity, hidden), BF16), pltpu.VMEM((capacity, experts), F32), pltpu.VMEM((tok, experts), F32),
                pltpu.VMEM((2, capacity, TILE), BF16), pltpu.VMEM((2, capacity, TILE), BF16),
                pltpu.VMEM((rows, hidden), F32), pltpu.VMEM((capacity, hidden), F32),
                pltpu.VMEM((n, 1, LANES), jnp.int32), pltpu.VMEM((LANES, LANES), F32),
                pltpu.VMEM((tok, 3 * experts), F32), pltpu.VMEM((tok, experts), BF16),
                pltpu.VMEM((half, 8, hidden // 2 + LANES), F32), pltpu.VMEM((half, 8, hidden // 2 + LANES), F32),
                pltpu.VMEM((8, hidden // 2 + LANES), F32), pltpu.VMEM((8, hidden // 2 + LANES), F32),
                pltpu.VMEM(chunk, F32), pltpu.VMEM((half,) + chunk, F32),
                dma((6,)), dma, dma, dma, dma((2 * n // GROUP,)), dma, dma, dma, dma((local_experts * n // GROUP,)),
                dma, dma, dma, dma, dma, dma, dma((4,)), dma((4,))],
            compiler_params=pltpu.CompilerParams(collective_id=0, has_side_effects=True, vmem_limit_bytes=41 * 1024 * 1024),
            name='moe',
        )(expert_picks, x, loss_w, gate_w.T, up_w, down_w)
        y, grad_x, grad_up, grad_down, grad_gate, loss = pl.pallas_call(
            flush_kernel,
            out_shape=[jax.ShapeDtypeStruct(v.shape, v.dtype) for v in held[:5]] + [jax.ShapeDtypeStruct((1, 1), F32)],
            in_specs=[vmem] * 6,
            out_specs=[hbm] * 5 + [pl.BlockSpec(memory_space=pltpu.SMEM)],
            scratch_shapes=[dma((9,))],
            compiler_params=pltpu.CompilerParams(vmem_limit_bytes=1024 * 1024),
            name='flush',
        )(*held)
        return y, loss[0, 0], grad_x, grad_up, grad_down, grad_gate.T

    return jax.shard_map(device_step, mesh=mesh,
                         in_specs=(P('ep'), P(), P('ep'), P('ep'), P('ep'), P('ep')),
                         out_specs=(P('ep'), P(), P('ep'), P('ep'), P('ep'), P()),
                         check_vma=False)
```

```python
import functools
import math
import jax
import jax.numpy as jnp
from jax import lax
from jax.experimental import pallas as pl
from jax.experimental.pallas import tpu as pltpu
from jax.sharding import PartitionSpec as P

F32 = jnp.float32
BF16 = jnp.bfloat16
GROUP = 8
TILE = 512
LANES = 128
C0 = math.sqrt(2.0 / math.pi)
C1 = 0.044715


def dot(a, b, ca=1, cb=0):
    return lax.dot_general(a, b, (((ca,), (cb,)), ((), ())), preferred_element_type=F32)


def split3(v):
    hi = v.astype(BF16)
    rest = v - hi.astype(F32)
    mid = rest.astype(BF16)
    return hi, mid, (rest - mid.astype(F32)).astype(BF16)


def softmax(logits):
    e = jnp.exp(logits - jnp.max(logits, axis=1, keepdims=True))
    return e / jnp.sum(e, axis=1, keepdims=True)


def xor(a, b, bits):
    return sum(((a // (1 << i) + b // (1 << i)) % 2) * (1 << i) for i in range(bits))


def moe_kernel(n, loss_scale, picks, x, r, gate_w, w1, w2,
               y_out, gx_out, w1_v, w2_v, gg_out, loss_out, u_far, da_far,
               picks_v, ids, wg, xr_v, pick, xr_s, xr_in, hs, h_in, gs, g_in, dh_v, s_in, s_own, u_t, da_t, acc, big,
               ids_in, ids_t, d_acc, dlog, red_s, red_in, swap_s, swap_in, all_s, all_in,
               load_sem, ids_ss, ids_rs, xr_ss, xr_rs, h_ss, h_rs, g_ss, g_rs, red_ss, red_rs, swap_ss, swap_rs, all_ss, all_rs, put_sem, get_sem):
    me = lax.axis_index('ep')
    bits = n.bit_length() - 1
    stages = n // GROUP
    half = n // 2
    tok, hidden = xr_v.shape[1:]
    per = tok // n
    rows = GROUP * per
    local_experts, _, ffn = w1_v.shape
    tiles = ffn // TILE
    experts = wg.shape[0]
    packed = LANES // per
    most = pl.ds(0, n - 1)

    def peer(p):
        return xor(me, n - 1 - p, bits)

    def group(i):
        return xor(me // GROUP, stages - 1 - i, bits - 3)

    def remote(src, dst, ss, rs, d):
        return pltpu.make_async_remote_copy(src, dst, ss, rs, device_id=(d,), device_id_type=pl.DeviceIdType.MESH)

    def span(q):
        return pl.ds(pl.multiple_of(q * rows, rows), rows)

    loads = [pltpu.make_async_copy(picks, picks_v, load_sem.at[4]), pltpu.make_async_copy(gate_w, wg, load_sem.at[5]),
             pltpu.make_async_copy(x, xr_v.at[0], load_sem.at[0]), pltpu.make_async_copy(r, xr_v.at[1], load_sem.at[1]),
             pltpu.make_async_copy(w1, w1_v, load_sem.at[2]), pltpu.make_async_copy(w2, w2_v, load_sem.at[3])]
    for c in loads:
        c.start()

    barrier = pltpu.get_barrier_semaphore()

    @pl.loop(0, n - 1)
    def _(p):
        pl.semaphore_signal(barrier, inc=1, device_id=(peer(p),), device_id_type=pl.DeviceIdType.MESH)

    loads[0].wait()
    for c in range(n // packed):
        ids[c] = picks_v[0:1, c * LANES:(c + 1) * LANES]
    pl.semaphore_wait(barrier, n - 1)

    @pl.loop(0, n - 1)
    def _(p):
        d = peer(p)
        remote(ids.at[d // packed], ids_in.at[me], ids_ss, ids_rs, d).start()
    ids_in[me] = ids[me // packed]
    all_ids = remote(ids_in.at[most], ids_in.at[most], ids_ss, ids_rs, me)
    all_ids.wait_send()
    all_ids.wait_recv()
    flat = ids_in[...].reshape(n, LANES).astype(F32)
    ids_t[...] = jnp.transpose(jnp.concatenate([flat] * (LANES // n), axis=0))
    cols = ids_t[pl.ds(pl.multiple_of((me % packed) * per, per), per), :]
    lane = lax.broadcasted_iota(jnp.int32, (per, LANES), 1)
    tok_iota = (lax.broadcasted_iota(jnp.int32, (per, tok), 1) + me * tok).astype(F32)

    for c in loads[1:4]:
        c.wait()

    def send_rows(s):
        w, i = s // stages, s % stages

        @pl.loop(0, GROUP)
        def _(j):
            p = i * GROUP + j

            @pl.when(p < n - 1)
            def _():
                d = peer(p)
                remote(xr_s.at[w, d], xr_in.at[w, me], xr_ss, xr_rs.at[s], d).start()

            @pl.when(p == n - 1)
            def _():
                xr_in[w, me] = xr_s[w, me]

    def gather_rows(s):
        w, q = s // stages, group(s % stages)
        xr_s[w, pl.ds(q * GROUP, GROUP)] = dot(pick[span(q), :], xr_v[w]).astype(BF16).reshape(GROUP, per, hidden)

    @pl.loop(0, stages)
    def _(s):
        base = group(s) * GROUP
        for j in range(GROUP):
            col = jnp.sum(jnp.where(lane == base + j, cols, 0.0), axis=1, keepdims=True)
            at = pl.multiple_of((base + j) * per, per)
            pick[pl.ds(at, per), :] = jnp.where(tok_iota == col, 1.0, 0.0).astype(BF16)

        @pl.when(s > 0)
        def _():
            send_rows(s - 1)
        gather_rows(s)

    @pl.loop(stages, 2 * stages)
    def _(s):
        gather_rows(s)
        send_rows(s - 1)

    @pl.loop(0, stages)
    def _(c):
        s_own[span(c), :] = softmax(dot(xr_v[0, span(c), :], wg[...], 1, 1))
    send_rows(2 * stages - 1)
    loads[4].wait()
    loads[5].wait()

    @pl.loop(0, stages * stages)
    def _(k):
        q, c = k // stages, k % stages

        @pl.when(c >= q)
        def _():
            upper = jnp.transpose(pick[span(q), span(c)].astype(F32)).astype(BF16)
            lower = jnp.transpose(pick[span(c), span(q)].astype(F32)).astype(BF16)
            pick[span(q), span(c)] = lower
            pick[span(c), span(q)] = upper

    def await_group(ref, sem, i):
        for cond, size in ((i < stages - 1, GROUP), (i == stages - 1, GROUP - 1)):
            @pl.when(cond)
            def _():
                part = ref(pl.ds(group(i) * GROUP, size))
                remote(part, part, xr_ss, sem, me).wait_recv()

    def send_h(i):
        @pl.loop(0, GROUP)
        def _(j):
            p = i * GROUP + j

            @pl.when(p < n - 1)
            def _():
                d = peer(p)
                remote(hs.at[d], h_in.at[me], h_ss, h_rs, d).start()

            @pl.when(p == n - 1)
            def _():
                h_in[me] = hs[me]

    lane_e = lax.broadcasted_iota(jnp.int32, (rows, experts), 1)
    row_dev = lax.broadcasted_iota(jnp.int32, (rows, experts), 0) // per

    @pl.loop(0, stages)
    def _(i):
        q = group(i)
        await_group(lambda b: xr_in.at[0, b], xr_rs.at[i], i)
        xg = xr_in[0, pl.ds(q * GROUP, GROUP)].reshape(rows, hidden)
        s_in[span(q), :] = softmax(dot(xg, wg[...], 1, 1))

        @pl.when(i > 0)
        def _():
            send_h(i - 1)

        @pl.loop(0, local_experts)
        def _(l):
            acc[...] = jnp.zeros_like(acc)

            @pl.loop(0, tiles, unroll=2)
            def _(t):
                at = pl.ds(pl.multiple_of(t * TILE, TILE), TILE)
                a = dot(xg, w1_v[l, :, at])
                u = (0.5 * a * (1.0 + jnp.tanh(C0 * (a + C1 * (a * a * a))))).astype(BF16)
                acc[...] += dot(u, w2_v[l, at, :])
            hs[pl.ds(q * GROUP, GROUP), pl.ds(pl.multiple_of(l * per, per), per), :] = acc[...].astype(BF16).reshape(GROUP, per, hidden)

    @pl.loop(0, stages)
    def _(i):
        await_group(lambda b: xr_in.at[1, b], xr_rs.at[stages + i], i)

        @pl.when(i == 0)
        def _():
            send_h(stages - 1)

    def wide_of(l):
        return pl.ds(pl.multiple_of(l * per, per), per)

    def send_g(l, i, lo, hi):
        @pl.loop(lo, hi)
        def _(j):
            p = i * GROUP + j

            @pl.when(p < n - 1)
            def _():
                d = peer(p)
                remote(gs.at[l, d], g_in.at[l, me], g_ss, g_rs.at[l * stages + i], d).start()

            @pl.when(p == n - 1)
            def _():
                g_in[l, me] = gs[l, me]

    def tile_at(t):
        return pl.ds(pl.multiple_of(t * TILE, TILE), TILE)

    def start_rows(l):
        @pl.loop(0, stages)
        def _(q):
            gate = jnp.sum(jnp.where(lane_e == me * local_experts + l, s_in[span(q), :], 0.0), axis=1, keepdims=True)
            dy = xr_in[1, pl.ds(q * GROUP, GROUP)].reshape(rows, hidden).astype(F32) * loss_scale
            dh_v[span(q), :] = (gate * dy).astype(BF16)
            big[span(q), :] = jnp.zeros((rows, hidden), F32)

    def row_grads(l, t, slot):
        at = tile_at(t)

        @pl.loop(0, stages, unroll=2)
        def _(q):
            up = w1_v[l, :, at]
            a = dot(xr_in[0, pl.ds(q * GROUP, GROUP)].reshape(rows, hidden), up)
            th = jnp.tanh(C0 * (a + C1 * (a * a * a)))
            side = 0.5 * (1.0 + th)
            u_t[slot, span(q), :] = (a * side).astype(BF16)
            slope = side + 0.5 * a * (1.0 - th * th) * (C0 + (3.0 * C0 * C1) * (a * a))
            du = dot(dh_v[span(q), :], w2_v[l, at, :], 1, 1).astype(BF16).astype(F32)
            da = (slope * du).astype(BF16)
            da_t[slot, span(q), :] = da
            big[span(q), :] += dot(da, up, 1, 1)

    def weight_grads(l, t, slot):
        at = tile_at(t)

        @pl.loop(0, TILE // rows)
        def _(m):
            part = dot(u_t[slot, :, span(m)], dh_v[...], 0, 0).astype(BF16)
            w2_v[l, pl.ds(pl.multiple_of(t * TILE + m * rows, rows), rows), :] = part

        @pl.loop(0, hidden // rows)
        def _(m):
            xm = xr_in[0, :, :, span(m)].reshape(tok, rows)
            w1_v[l, span(m), at] = dot(xm, da_t[slot], 0, 0).astype(BF16)

    def finish_rows(l):
        @pl.loop(0, stages)
        def _(q):
            gs[l, pl.ds(q * GROUP, GROUP)] = big[span(q), :].astype(BF16).reshape(GROUP, per, hidden)

    last = local_experts - 1

    @pl.loop(0, last)
    def _(l):
        start_rows(l)

        @pl.loop(0, tiles)
        def _(t):
            row_grads(l, t, 0)
            weight_grads(l, t, 0)
        finish_rows(l)

        @pl.loop(0, stages)
        def _(i):
            send_g(l, i, 0, GROUP)

    def aside(t, slot):
        return (pltpu.make_async_copy(u_t.at[slot], u_far.at[t], put_sem.at[slot]),
                pltpu.make_async_copy(da_t.at[slot], da_far.at[t], put_sem.at[2 + slot]))

    def fetch(t, slot):
        return (pltpu.make_async_copy(u_far.at[t], u_t.at[slot], get_sem.at[slot]),
                pltpu.make_async_copy(da_far.at[t], da_t.at[slot], get_sem.at[2 + slot]))

    start_rows(last)

    @pl.loop(0, tiles)
    def _(t):
        slot = t % 2

        @pl.when(t >= 2)
        def _():
            for c in aside(t - 2, slot):
                c.wait()
        row_grads(last, t, slot)

        @pl.when(t < tiles - 2)
        def _():
            for c in aside(t, slot):
                c.start()
    finish_rows(last)
    for slot in range(2):
        weight_grads(last, tiles - 2 + slot, slot)
        if slot == 0:
            @pl.loop(2, stages)
            def _(i):
                send_g(last, i, 0, GROUP)
            send_g(last, 0, 0, GROUP)
        for c in fetch(slot, slot):
            c.start()

    all_h = remote(hs.at[most], h_in.at[most], h_ss, h_rs, me)
    all_h.wait_recv()

    @pl.loop(0, stages)
    def _(q):
        big[span(q), :] = xr_v[0, span(q), :].astype(F32)
        d_acc[span(q), :] = jnp.zeros((rows, 3 * experts), F32)

    @pl.loop(0, stages)
    def _(q):
        blocks = pl.ds(q * GROUP, GROUP)
        slot_probs = softmax(dot(xr_s[0, blocks].reshape(rows, hidden), wg[...], 1, 1))
        dy = xr_s[1, blocks].reshape(rows, hidden).astype(F32) * loss_scale
        mixed, d_slot = 0.0, 0.0
        for l in range(local_experts):
            here = lane_e == (q * GROUP + row_dev) * local_experts + l
            h = h_in[blocks, l * per:(l + 1) * per, :].reshape(rows, hidden).astype(F32)
            mixed += jnp.sum(jnp.where(here, slot_probs, 0.0), axis=1, keepdims=True) * h
            d_slot += jnp.where(here, jnp.sum(dy * h, axis=1, keepdims=True), 0.0)
        m3 = jnp.concatenate(split3(mixed), axis=0)
        d3 = jnp.concatenate(split3(d_slot), axis=1)

        @pl.loop(0, stages)
        def _(c):
            p = pick[span(c), span(q)]
            big[span(c), :] += dot(jnp.concatenate([p, p, p], axis=1), m3)
            d_acc[span(c), :] += dot(p, d3)

    acc[pl.ds(0, 8), pl.ds(0, LANES)] = jnp.zeros((8, LANES), F32)
    big_g = acc.at[pl.ds(64, experts), :]
    big_g[...] = jnp.zeros((experts, hidden), F32)

    @pl.loop(0, stages)
    def _(c):
        y = big[span(c), :].astype(BF16)
        y_out[span(c), :] = y
        lost = jnp.sum(y.astype(F32) * xr_v[1, span(c), :].astype(F32), axis=0, keepdims=True)
        acc[pl.ds(0, 1), pl.ds(0, LANES)] += jnp.broadcast_to(jnp.sum(lost, axis=1, keepdims=True), (1, LANES))
        d3 = d_acc[span(c), :]
        d_probs = d3[:, :experts] + d3[:, experts:2 * experts] + d3[:, 2 * experts:]
        probs = s_own[span(c), :]
        dl = (probs * (d_probs - jnp.sum(probs * d_probs, axis=1, keepdims=True))).astype(BF16)
        dlog[span(c), :] = dl
        big_g[...] += dot(dl, xr_v[0, span(c), :], 0, 0)

    wide = hidden // 2
    lost = jnp.broadcast_to(acc[pl.ds(0, 1), pl.ds(0, LANES)], (8, LANES)) * loss_scale
    for c in range(half):
        red_s[c, :, :wide] = big_g[8 * (c // 2):8 * (c // 2) + 8, wide * (c % 2):wide * (c % 2) + wide]
        red_s[c, :, wide:] = lost
    mine = me % half
    red_in[mine] = red_s[mine]

    @pl.loop(0, stages)
    def _(c):
        big[span(c), :] = xr_v[1, span(c), :].astype(F32) * loss_scale + dot(dlog[span(c), :], wg[...], 1, 0)

    @pl.loop(half, n - 1)
    def _(p):
        d = peer(p)
        remote(red_s.at[d % half], red_in.at[mine], red_ss, red_rs, d).start()
    send_g(last, 1, 0, GROUP // 2)

    @pl.loop(0, tiles - 2)
    def _(t):
        slot = t % 2
        for c in fetch(t, slot):
            c.wait()
        weight_grads(last, t, slot)

        @pl.when(t < tiles - 4)
        def _():
            for c in fetch(t + 2, slot):
                c.start()

    def add_g(l, i):
        await_group(lambda b: g_in.at[l, b], g_rs.at[l * stages + i], i)
        q = group(i)
        g = g_in[l, pl.ds(q * GROUP, GROUP)].reshape(rows, hidden)

        @pl.loop(0, stages)
        def _(c):
            big[span(c), :] += dot(pick[span(c), span(q)], g)

    some = pl.ds(0, half - 1)
    red = remote(red_s.at[some], red_in.at[some], red_ss, red_rs, me)
    red.wait_recv()
    swap_s[...] = jnp.sum(red_in[...], axis=0)
    add_g(0, 0)
    swap = remote(swap_s, swap_in, swap_ss, swap_rs, peer(half - 1))
    swap.start()
    send_g(last, 1, GROUP // 2, GROUP)

    @pl.loop(1, last * stages)
    def _(s):
        add_g(s // stages, s % stages)
    add_g(last, 2)
    swap.wait_recv()
    full = swap_s[...] + swap_in[...]
    loss_out[...] = full[:, wide:]
    all_s[...] = full[:, :wide]
    all_in[mine] = full[:, :wide]
    add_g(last, 3)

    @pl.loop(half, n - 1)
    def _(p):
        remote(all_s, all_in.at[mine], all_ss, all_rs, peer(p)).start()
    add_g(last, 0)
    await_group(lambda b: g_in.at[last, b], g_rs.at[last * stages + 1], 1)
    end = group(1)
    g_end = g_in[last, pl.ds(end * GROUP, GROUP)].reshape(rows, hidden)

    @pl.loop(0, stages, unroll=2)
    def _(c):
        gx_out[span(c), :] = (big[span(c), :] + dot(pick[span(c), span(end)], g_end)).astype(BF16)
    gathered = remote(all_in.at[some], all_in.at[some], all_ss, all_rs, me)
    gathered.wait_recv()
    for c in range(half):
        gg_out[8 * (c // 2):8 * (c // 2) + 8, wide * (c % 2):wide * (c % 2) + wide] = all_in[c]
    swap.wait_send()
    red.wait_send()
    gathered.wait_send()
    all_h.wait_send()
    for w in range(2):
        remote(xr_s.at[w, most], xr_in.at[w, most], xr_ss, xr_rs.at[0], me).wait_send()
    for l in range(local_experts):
        remote(gs.at[l, most], g_in.at[l, most], g_ss, g_rs.at[0], me).wait_send()


def flush_kernel(y, gx, gu, gd, gg, loss, y_out, gx_out, gu_out, gd_out, gg_out, loss_out, sem):
    parts = [(gu.at[l], gu_out.at[l]) for l in range(gu.shape[0])] + [(gd.at[l], gd_out.at[l]) for l in range(gd.shape[0])]
    parts += [(y, y_out), (gx, gx_out), (gg, gg_out)]
    copies = [pltpu.make_async_copy(a, b, sem.at[k]) for k, (a, b) in enumerate(parts)]
    for c in copies:
        c.start()
    loss_out[0, 0] = loss[0, 0]
    for c in copies:
        c.wait()


def solution(mesh):
    n = mesh.shape['ep']

    def device_step(x, gate_w, up_w, down_w, expert_picks, loss_w):
        tok, hidden = x.shape
        local_experts, capacity = expert_picks.shape
        per = capacity // n
        experts = gate_w.shape[1]
        loss_scale = 1.0 / math.sqrt(tok * n * hidden)
        rows = GROUP * per
        half = n // 2
        hbm = pl.BlockSpec(memory_space=pl.ANY)
        vmem = pl.BlockSpec(memory_space=pltpu.VMEM)
        dma = pltpu.SemaphoreType.DMA
        blocks = (n, per, hidden)
        wide = (n, local_experts * per, hidden)
        chunk = (8, hidden // 2)
        flat = pltpu.VMEM(x.shape, BF16)
        aside = jax.ShapeDtypeStruct((up_w.shape[2] // TILE, capacity, TILE), BF16)
        *held, _, _ = pl.pallas_call(
            functools.partial(moe_kernel, n, loss_scale),
            out_shape=[flat, flat, pltpu.VMEM(up_w.shape, BF16), pltpu.VMEM(down_w.shape, BF16),
                       pltpu.VMEM((experts, hidden), F32), pltpu.VMEM((8, LANES), F32)] + [aside] * 2,
            in_specs=[hbm] * 6,
            out_specs=[vmem] * 6 + [hbm] * 2,
            scratch_shapes=[
                pltpu.VMEM(expert_picks.shape, jnp.int32), pltpu.VMEM((capacity // LANES, 1, LANES), jnp.int32),
                pltpu.VMEM((experts, hidden), BF16), pltpu.VMEM((2, tok, hidden), BF16),
                pltpu.VMEM((capacity, tok), BF16), pltpu.VMEM((2,) + blocks, BF16), pltpu.VMEM((2,) + blocks, BF16),
                pltpu.VMEM(wide, BF16), pltpu.VMEM(wide, BF16),
                pltpu.VMEM((local_experts,) + blocks, BF16), pltpu.VMEM((local_experts,) + blocks, BF16),
                pltpu.VMEM((capacity, hidden), BF16), pltpu.VMEM((capacity, experts), F32), pltpu.VMEM((tok, experts), F32),
                pltpu.VMEM((2, capacity, TILE), BF16), pltpu.VMEM((2, capacity, TILE), BF16),
                pltpu.VMEM((rows, hidden), F32), pltpu.VMEM((capacity, hidden), F32),
                pltpu.VMEM((n, 1, LANES), jnp.int32), pltpu.VMEM((LANES, LANES), F32),
                pltpu.VMEM((tok, 3 * experts), F32), pltpu.VMEM((tok, experts), BF16),
                pltpu.VMEM((half, 8, hidden // 2 + LANES), F32), pltpu.VMEM((half, 8, hidden // 2 + LANES), F32),
                pltpu.VMEM((8, hidden // 2 + LANES), F32), pltpu.VMEM((8, hidden // 2 + LANES), F32),
                pltpu.VMEM(chunk, F32), pltpu.VMEM((half,) + chunk, F32),
                dma((6,)), dma, dma, dma, dma((2 * n // GROUP,)), dma, dma, dma, dma((local_experts * n // GROUP,)),
                dma, dma, dma, dma, dma, dma, dma((4,)), dma((4,))],
            compiler_params=pltpu.CompilerParams(collective_id=0, has_side_effects=True, vmem_limit_bytes=41 * 1024 * 1024),
            name='moe',
        )(expert_picks, x, loss_w, gate_w.T, up_w, down_w)
        y, grad_x, grad_up, grad_down, grad_gate, loss = pl.pallas_call(
            flush_kernel,
            out_shape=[jax.ShapeDtypeStruct(v.shape, v.dtype) for v in held[:5]] + [jax.ShapeDtypeStruct((1, 1), F32)],
            in_specs=[vmem] * 6,
            out_specs=[hbm] * 5 + [pl.BlockSpec(memory_space=pltpu.SMEM)],
            scratch_shapes=[dma((9,))],
            compiler_params=pltpu.CompilerParams(vmem_limit_bytes=1024 * 1024),
            name='flush',
        )(*held)
        return y, loss[0, 0], grad_x, grad_up, grad_down, grad_gate.T

    return jax.shard_map(device_step, mesh=mesh,
                         in_specs=(P('ep'), P(), P('ep'), P('ep'), P('ep'), P('ep')),
                         out_specs=(P('ep'), P(), P('ep'), P('ep'), P('ep'), P()),
                         check_vma=False)
```
